32 devices in a mesh: dp: 2 (over y), seq: 16 (over z, x, core).
Axes of the slice: x: 2, y: 2, z: 4, core: 2. Of those that a mesh axis runs over, the one named last changes fastest.
Arguments:
- features: bfloat16 [4096, 320], P(('dp', 'seq')), parts along dimension 0, may hold values from -40 to 40
- hint: bfloat16 [4096, 320], P(('dp', 'seq')), parts along dimension 0, may hold values from -6 to 6
- conv_weight: bfloat16 [3, 3, 320, 320], replicated, may hold values from -0.109375 to 0.109375
- conv_bias: float32 [320], replicated, may hold values from -3 to 3
- zero_weight: bfloat16 [320, 320], replicated, may hold values from -0.3125 to 0.3125
- zero_bias: float32 [320], replicated, may hold values from -2 to 2
- group_gain: float32 [320], replicated, may hold values from 0.5 to 1.5
- proj_in: bfloat16 [320, 320], replicated, may hold values from -0.3125 to 0.3125
- norm_gain: float32 [320], replicated, may hold values from 0.5 to 1.5
- query_weight: bfloat16 [320, 320], replicated, may hold values from -2 to 2
- key_weight: bfloat16 [320, 320], replicated, may hold values from -2 to 2
- value_weight: bfloat16 [320, 320], replicated, may hold values from -0.3125 to 0.3125
- attn_out: bfloat16 [320, 320], replicated, may hold values from -0.3125 to 0.3125
- proj_out: bfloat16 [320, 320], replicated, may hold values from -0.3125 to 0.3125
Outputs:
- block_out: bfloat16 [4096, 320], P(('dp', 'seq')), parts along dimension 0
The draws below stay inside these ranges and needn't reach their ends.
There are 2 independent parts, one for each index of `dp`. The reference program is written for one: setup_inputs(seed, part) draws one part's arguments, and reference() takes and returns one part's arrays. A program takes and returns all parts, laid end to end along the dimension named above; an argument that names none is the same for every part. Nothing has to cross between parts.
All inputs are finite; a program needn't handle non-finite values.
Results may differ from the reference program's by a relative error of at most 0.023.
Values may be sent and summed in bfloat16 or wider, within the bound.
A program may use at most 64 MiB of HBM per device.

```python
import math
import jax
import jax.numpy as jnp
from jax import lax

C = 320
HEADS = 8
GROUPS = 32
WIDTH = 128
SEQ = 2048


def draw_features(key, part):
    sub_keys = [jax.random.fold_in(key, 11 + index) for index in range(8)]
    position = jnp.arange(SEQ, dtype=jnp.float32) / (SEQ - 1)
    noise_vals = jnp.clip(jax.random.normal(sub_keys[0], (SEQ, C), jnp.float32), -4.0, 4.0)
    rise_row = 1.0 + 2.0 * position
    row_scale = jnp.exp(jax.random.uniform(sub_keys[1], (SEQ,), jnp.float32, math.log(0.3), 0.0))
    col_scale = jnp.exp(jax.random.uniform(sub_keys[2], (C,), jnp.float32, math.log(0.5), math.log(2.0)))
    group_off = jax.random.normal(sub_keys[4], (GROUPS,), jnp.float32)
    offset_col = jnp.repeat(group_off, C // GROUPS) + 0.3 * jax.random.normal(sub_keys[3], (C,), jnp.float32)
    offset_rise = 0.3 + 2.7 * position
    drawn = offset_rise[:, None] * offset_col[None, :] + (rise_row * row_scale)[:, None] * col_scale[None, :] * noise_vals
    return jnp.clip(drawn, -40.0, 40.0).astype(jnp.bfloat16)


def draw_hint(key, part):
    sub_keys = [jax.random.fold_in(key, 41 + index) for index in range(6)]
    position = jnp.arange(SEQ, dtype=jnp.float32) / (SEQ - 1)
    sign_col = jnp.where(jax.random.bernoulli(sub_keys[0], 0.5, (C,)), 1.0, -1.0)
    ramp_size = jax.random.uniform(sub_keys[1], (C,), jnp.float32, 0.5, 1.5)
    offset_col = 1.5 * jax.random.normal(sub_keys[2], (C,), jnp.float32)
    noise_vals = jnp.clip(jax.random.normal(sub_keys[3], (SEQ, C), jnp.float32), -4.0, 4.0)
    ramp_amp = 2.5
    ramp = ramp_amp * (2.0 * position - 1.0)
    drawn = offset_col[None, :] + ramp[:, None] * (sign_col * ramp_size)[None, :] + noise_vals
    return jnp.clip(drawn, -6.0, 6.0).astype(jnp.bfloat16)


def weight_pair(key):
    base_key = jax.random.fold_in(key, 71)
    first_mat = jax.random.normal(jax.random.fold_in(base_key, 1), (C, C), jnp.float32)
    second_mat = jax.random.normal(jax.random.fold_in(base_key, 2), (C, C), jnp.float32)
    query_mat = first_mat * (1.5 / math.sqrt(C))
    key_mat = -(first_mat + 0.3 * second_mat) * (1.5 / math.sqrt(C))
    return (jnp.clip(query_mat, -2.0, 2.0), jnp.clip(key_mat, -2.0, 2.0))


def draw_query_weight(key, part):
    return weight_pair(key)[0].astype(jnp.bfloat16)


def draw_key_weight(key, part):
    return weight_pair(key)[1].astype(jnp.bfloat16)


def bell_draw(key, dims, scale, limit, kind=jnp.bfloat16):
    array = scale * jax.random.normal(key, dims, jnp.float32)
    return jnp.clip(array, min=-limit, max=limit).astype(kind)


def setup_inputs(seed: int = 0, part: int = 0) -> dict:
    keys = jax.random.split(jax.random.key(seed), 15)
    own_keys = jax.random.split(jax.random.fold_in(keys[14], part), 15)
    return {
        "features": draw_features(jax.random.fold_in(jax.random.fold_in(keys[14], part), 71), part),
        "hint": draw_hint(jax.random.fold_in(jax.random.fold_in(keys[14], part), 71), part),
        "conv_weight": bell_draw(keys[2], (3, 3, C, C), (9 * C) ** -0.5, 0.109375),
        "conv_bias": bell_draw(keys[3], (C,), 0.5, 3.0, jnp.float32),
        "zero_weight": bell_draw(keys[4], (C, C), C ** -0.5, 0.3125),
        "zero_bias": bell_draw(keys[5], (C,), 0.3, 2.0, jnp.float32),
        "group_gain": jnp.clip(1.0 + 0.1 * jax.random.normal(keys[6], (C,), jnp.float32), 0.5, 1.5),
        "proj_in": bell_draw(keys[7], (C, C), C ** -0.5, 0.3125),
        "norm_gain": jnp.clip(1.0 + 0.1 * jax.random.normal(keys[8], (C,), jnp.float32), 0.5, 1.5),
        "query_weight": draw_query_weight(jax.random.fold_in(keys[14], 71), part),
        "key_weight": draw_key_weight(jax.random.fold_in(keys[14], 71), part),
        "value_weight": bell_draw(keys[11], (C, C), C ** -0.5, 0.3125),
        "attn_out": bell_draw(keys[12], (C, C), C ** -0.5, 0.3125),
        "proj_out": bell_draw(keys[13], (C, C), C ** -0.5, 0.3125),
    }


norm_eps = 1e-06
layer_eps = 1e-05

def conv_extended(extended, conv_weight, conv_bias, width):
    line_count = extended.shape[0] // width - 2
    channels = extended.shape[1]
    lattice = extended.reshape(line_count + 2, width, channels)
    padded = jnp.pad(lattice, ((0, 0), (1, 1), (0, 0)))
    summed = jnp.zeros((line_count * width, conv_weight.shape[3]), jnp.float32)
    for row_shift in range(3):
        for col_shift in range(3):
            window = padded[row_shift:row_shift + line_count, col_shift:col_shift + width]
            window = window.reshape(line_count * width, channels)
            summed = summed + jnp.dot(window, conv_weight[row_shift, col_shift], preferred_element_type=jnp.float32)
    return summed + conv_bias

def control_merge(features, extended, conv_weight, conv_bias, zero_weight, zero_bias):
    control = jax.nn.silu(conv_extended(extended, conv_weight, conv_bias, WIDTH)).astype(jnp.bfloat16)
    branch = jnp.dot(control, zero_weight, preferred_element_type=jnp.float32) + zero_bias
    return (features.astype(jnp.float32) + branch).astype(jnp.bfloat16)

def group_apply(merged, mean_group, var_group, group_gain):
    per_group = merged.shape[1] // mean_group.shape[0]
    mean_chan = jnp.repeat(mean_group, per_group)
    inv_chan = jnp.repeat(lax.rsqrt(var_group + norm_eps), per_group)
    return ((merged.astype(jnp.float32) - mean_chan) * inv_chan * group_gain).astype(jnp.bfloat16)

def project_norm(grouped, proj_in, norm_gain):
    inner_rows = jnp.dot(grouped, proj_in, preferred_element_type=jnp.float32).astype(jnp.bfloat16)
    widened = inner_rows.astype(jnp.float32)
    centre = lax.optimization_barrier(jnp.mean(widened, axis=1, keepdims=True))
    spread = lax.optimization_barrier(jnp.mean(jnp.square(widened - centre), axis=1, keepdims=True))
    normed = ((widened - centre) * lax.rsqrt(spread + layer_eps) * norm_gain).astype(jnp.bfloat16)
    return (inner_rows, normed)

def reference(features, hint, conv_weight, conv_bias, zero_weight, zero_bias, group_gain, proj_in, norm_gain, query_weight, key_weight, value_weight, attn_out, proj_out):
    seq_len, channels = features.shape
    extended = jnp.pad(hint, ((WIDTH, WIDTH), (0, 0)))
    merged = control_merge(features, extended, conv_weight, conv_bias, zero_weight, zero_bias)
    widened = merged.astype(jnp.float32)
    per_group = channels // GROUPS
    entry_count = seq_len * per_group
    mean_group = lax.optimization_barrier(jnp.sum(widened.reshape(seq_len, GROUPS, per_group), axis=(0, 2))) / entry_count
    centred = widened - jnp.repeat(mean_group, per_group)
    var_group = lax.optimization_barrier(jnp.sum(jnp.square(centred).reshape(seq_len, GROUPS, per_group), axis=(0, 2))) / entry_count
    grouped = group_apply(merged, mean_group, var_group, group_gain)
    inner_rows, normed = project_norm(grouped, proj_in, norm_gain)
    head_dim = channels // HEADS

    def project(weight):
        made = jnp.dot(normed, weight, preferred_element_type=jnp.float32).astype(jnp.bfloat16)
        return made.reshape(seq_len, HEADS, head_dim)
    queries = project(query_weight)
    keys_wide = project(key_weight).astype(jnp.float32)
    values_wide = project(value_weight).astype(jnp.float32)
    block_len = math.gcd(seq_len, 512)
    score_scale = 1.0 / math.sqrt(head_dim)

    def attend(query_block):
        scores = jnp.einsum('qhd,khd->hqk', query_block.astype(jnp.float32), keys_wide) * score_scale
        row_max = lax.optimization_barrier(jnp.max(scores, axis=2, keepdims=True))
        weights = jnp.exp(scores - row_max)
        running_sum = lax.optimization_barrier(jnp.sum(weights, axis=2))
        rounded = lax.optimization_barrier(weights.astype(jnp.bfloat16)).astype(jnp.float32)
        weighted = jnp.einsum('hqk,khd->qhd', rounded, values_wide)
        return weighted / jnp.transpose(running_sum)[:, :, None]
    blocks = queries.reshape(seq_len // block_len, block_len, HEADS, head_dim)
    attended = lax.map(attend, blocks).reshape(seq_len, channels).astype(jnp.bfloat16)
    after_attn = (inner_rows.astype(jnp.float32) + jnp.dot(attended, attn_out, preferred_element_type=jnp.float32)).astype(jnp.bfloat16)
    return (merged.astype(jnp.float32) + jnp.dot(after_attn, proj_out, preferred_element_type=jnp.float32)).astype(jnp.bfloat16)
```

```python
import functools
import math

import jax
import jax.numpy as jnp
from jax import lax
from jax.experimental import pallas as pl
from jax.experimental.pallas import tpu as pltpu
from jax.sharding import PartitionSpec as P

HEADS = 8
GROUPS = 32
WIDTH = 128
CORES = 2
LANES = 128
PIECES = 2
PLAN = (
    "r1", "s", "q", "x0", "k0", "r2", "o0", "w0", "x1", "k1", "r3", "p0o1", "x2", "k2",
    "w1", "p1o2", "x3", "k3", "w2", "p2o3", "w3", "p3",
)
EARLY = ()
SENDS = ("3","1","s")

norm_eps = 1e-06
layer_eps = 1e-05
MESH = pl.DeviceIdType.MESH
F32 = jnp.float32
BF16 = jnp.bfloat16
LOWEST = -3.0e38


def mm(x, y):
    return jnp.dot(x, y, preferred_element_type=F32)


def mm_t(x, y):
    return lax.dot_general(x, y, (((1,), (1,)), ((), ())), preferred_element_type=F32)


def split3(x):
    hi = x.astype(BF16)
    rest = x - hi.astype(F32)
    mid = rest.astype(BF16)
    lo = (rest - mid.astype(F32)).astype(BF16)
    return hi, mid, lo


def row_order(rows_a):
    return [sorted(range(rows_a), key=lambda aa: (abs(aa - a), abs(2 * aa - rows_a + 1))) for a in range(rows_a)]


def block_kernel(
    n, rows_a, rows_b,
    features_hbm, hint_hbm, conv_bias_hbm, zero_bias_hbm, group_gain_hbm, norm_gain_hbm,
    conv_hbm, zero_hbm, proj_in_hbm, query_hbm, key_hbm, value_hbm, attn_hbm, proj_hbm,
    out,
    features, hint, conv_bias, zero_bias, group_gain, norm_gain,
    conv_w, zero_w, proj_in_w, query_w, key_w, value_w, attn_w, proj_w,
    halo, gathered, kbuf, vbuf, qbd, stats, same, expand, zero_col, gain_col, layer_col, mean_bc, inv_bc,
    inner_own, top, total, acc,
    load_sem, halo_send, halo_recv, token, stat_send, stat_recv, send_sem, recv_sem, kv_send, kv_recv,
):
    channels, tokens = out.shape
    head_dim = channels // HEADS
    per_group = channels // GROUPS
    pairs = HEADS // 2
    pair_dim = 2 * head_dim
    me = lax.axis_index("seq")
    core = lax.rem(me, CORES)
    chip = lax.div(me, CORES)
    b = lax.rem(chip, rows_b)
    a = lax.div(chip, rows_b)

    def device(aa, bb, cc):
        return (aa * rows_b + bb) * CORES + cc

    loads = {}
    for slot, (name, src, dst) in enumerate((
        ("hint", hint_hbm, hint), ("conv", conv_hbm, conv_w), ("zero", zero_hbm, zero_w),
        ("features", features_hbm, features), ("conv_bias", conv_bias_hbm, conv_bias),
        ("zero_bias", zero_bias_hbm, zero_bias), ("group_gain", group_gain_hbm, group_gain),
        ("norm_gain", norm_gain_hbm, norm_gain), ("proj_in", proj_in_hbm, proj_in_w),
        ("query", query_hbm, query_w), ("key", key_hbm, key_w), ("value", value_hbm, value_w),
        ("attn", attn_hbm, attn_w), ("proj", proj_hbm, proj_w),
    )):
        loads[name] = pltpu.make_async_copy(src, dst, load_sem.at[slot])
        loads[name].start()

    pending = []

    def when(cond, fn):
        if cond is None:
            fn()
        else:
            pl.when(cond)(fn)

    def signal(sem, peer):
        pl.semaphore_signal(sem, inc=1, device_id={"seq": peer}, device_id_type=MESH)

    up, down = a < rows_a - 1, a > 0

    def as_int(cond):
        return cond.astype(jnp.int32)

    barrier = pltpu.get_barrier_semaphore()
    last_in_row = (b == rows_b - 1) & (core == 1) & up
    first_in_row = (b == 0) & (core == 0) & down
    mates = [(k, j) for k in range(rows_b) for j in range(CORES) if (k, j) != (0, 0)]
    for k, j in mates:
        signal(barrier, device(a, lax.rem(b + k, rows_b), lax.rem(core + j, CORES)))
    for cond, peer in ((up, device(a + 1, b, core)), (down, device(a - 1, b, core)),
                       (last_in_row, me + 1), (first_in_row, me - 1)):
        when(cond, functools.partial(signal, barrier, peer))
    pl.semaphore_wait(barrier, len(mates) + as_int(up) + as_int(down) + as_int(last_in_row) + as_int(first_in_row))

    loads["hint"].wait()
    to_next = pltpu.make_async_remote_copy(
        hint.at[:, pl.ds(tokens - WIDTH, WIDTH)], halo.at[0], halo_send.at[0], halo_recv.at[0], device_id={"seq": me + 1}, device_id_type=MESH)
    to_prev = pltpu.make_async_remote_copy(
        hint.at[:, pl.ds(0, WIDTH)], halo.at[1], halo_send.at[1], halo_recv.at[1], device_id={"seq": me - 1}, device_id_type=MESH)
    pl.when(me < n - 1)(to_next.start)
    pl.when(me > 0)(to_prev.start)

    when(up, functools.partial(signal, token.at[0], device(a + 1, b, core)))
    when(down, functools.partial(signal, token.at[0], device(a - 1, b, core)))

    @pl.when(me == 0)
    def _():
        halo[0] = jnp.zeros((channels, WIDTH), BF16)

    @pl.when(me == n - 1)
    def _():
        halo[1] = jnp.zeros((channels, WIDTH), BF16)

    row_group = lax.div(lax.broadcasted_iota(jnp.int32, (channels, channels), 0), jnp.int32(per_group))
    col_group = lax.div(lax.broadcasted_iota(jnp.int32, (channels, channels), 1), jnp.int32(per_group))
    same[...] = (row_group == col_group).astype(BF16)
    expand[...] = (
        lax.div(lax.broadcasted_iota(jnp.int32, (channels, LANES), 0), jnp.int32(per_group))
        == lax.broadcasted_iota(jnp.int32, (channels, LANES), 1)).astype(BF16)

    def as_columns(vector):
        return jnp.transpose(jnp.broadcast_to(vector[...].reshape(1, channels), (LANES, channels)))

    loads["conv"].wait()
    middle = jnp.transpose(hint[...])
    taps = [mm(middle, conv_w[1, d]) for d in range(3)]
    for name in ("zero", "features", "conv_bias", "zero_bias", "group_gain", "norm_gain"):
        loads[name].wait()
    zero_w[...] = jnp.transpose(zero_w[...])
    zero_col[...] = as_columns(zero_bias)
    gain_col[...] = as_columns(group_gain)
    layer_col[...] = as_columns(norm_gain)
    for name in ("proj_in", "query", "key", "value", "attn", "proj"):
        loads[name].wait()
    for weight in (proj_in_w, query_w, key_w, value_w, attn_w, proj_w):
        weight[...] = jnp.transpose(weight[...])

    pl.semaphore_wait(token.at[0], as_int(up) + as_int(down))
    up2, down2 = a + 2 < rows_a, a >= 2
    when(up2, functools.partial(signal, token.at[1], device(a + 2, b, core)))
    when(down2, functools.partial(signal, token.at[1], device(a - 2, b, core)))

    pl.when(me > 0)(to_next.wait_recv)
    pl.when(me < n - 1)(to_prev.wait_recv)
    for k, dy in enumerate((0, 2)):
        line = jnp.transpose(halo[k])
        if tokens > WIDTH:
            line = jnp.concatenate([line, middle[:-WIDTH]] if k == 0 else [middle[WIDTH:], line], axis=0)
        taps = [taps[d] + mm(line, conv_w[dy, d]) for d in range(3)]
    column = lax.rem(lax.broadcasted_iota(jnp.int32, (tokens, channels), 0), WIDTH)
    left = jnp.where(column == 0, 0.0, pltpu.roll(taps[0], 1, 0))
    right = jnp.where(column == WIDTH - 1, 0.0, pltpu.roll(taps[2], tokens - 1, 0))
    conv = left + taps[1] + right + conv_bias[...].reshape(1, channels)
    control = (conv / (1.0 + jnp.exp(-conv))).astype(BF16)
    branch = mm_t(zero_w[...], control) + zero_col[...]
    merged = (features[...].astype(F32) + branch).astype(BF16)
    gathered[a, b] = merged

    part = channels // PIECES

    def piece(aa, bb, h):
        return gathered.at[aa, bb, pl.ds(h * part, part)]

    def send(aa, bb, h, target, cond):
        slot = len(pending)
        copy = pltpu.make_async_remote_copy(
            piece(aa, bb, h), piece(aa, bb, h), send_sem.at[slot], recv_sem.at[aa, bb, h],
            device_id={"seq": target}, device_id_type=MESH)
        pending.append((cond, copy))
        when(cond, copy.start)

    def arrive(aa, bb, h):
        pltpu.make_async_remote_copy(
            piece(aa, bb, h), piece(aa, bb, h), send_sem.at[0], recv_sem.at[aa, bb, h],
            device_id={"seq": me}, device_id_type=MESH).wait_recv()

    def across(aa, h, cond):
        for k in range(1, rows_b):
            send(aa, b, h, device(a, lax.rem(b + k, rows_b), core), cond)

    def relay(step):
        for h in range(PIECES):
            for sign, inside, more in ((1, a + step < rows_a, down), (-1, a >= step, up)):
                aa = a + sign * step
                pl.when(inside)(functools.partial(arrive, aa, b, h))
                if step + 1 < rows_a and str(step + 1) not in EARLY + SENDS:
                    send(aa, b, h, device(a - sign, b, core), inside & more)
                if str(step) + "x" not in EARLY + SENDS:
                    across(aa, h, inside)

    def direct(step, columns):
        for h in range(PIECES):
            for sign, inside in ((-1, a >= step), (1, a + step < rows_a)):
                for k in columns:
                    send(a, b, h, device(a + sign * step, lax.rem(b + k, rows_b), core), inside)

    def launch(words):
        for word in words:
            if word == "s":
                for h in range(PIECES):
                    across(a, h, None)
            else:
                direct(int(word[0]), range(1, rows_b) if word[1:] else range(1))

    launch(EARLY)

    by_token = jnp.transpose(merged).astype(F32)
    shift = by_token[:1]
    apart = by_token - shift
    first = jnp.sum(apart, axis=0, keepdims=True)
    second = jnp.sum(apart * apart, axis=0, keepdims=True)
    channel_mean = shift + first * (1.0 / tokens)
    channel_dev = jnp.maximum(second - first * first * (1.0 / tokens), 0.0)

    def stack_rows(rows):
        fill = 16 - len(rows)
        return jnp.concatenate(rows + [jnp.zeros((fill,) + rows[0].shape[1:], BF16)], axis=0)

    spread = mm(stack_rows(list(split3(channel_mean))), same[...])
    group_mean = jnp.sum(spread[:3], axis=0, keepdims=True) * (1.0 / per_group)
    off = channel_mean - group_mean
    group_dev = channel_dev + tokens * off * off
    packed = mm(stack_rows(list(split3(channel_mean)) + list(split3(group_dev))), expand[...])
    stats[me] = jnp.concatenate([
        jnp.sum(packed[:3], axis=0, keepdims=True) * (1.0 / per_group),
        jnp.sum(packed[3:6], axis=0, keepdims=True)], axis=0)

    pl.semaphore_wait(token.at[1], as_int(up2) + as_int(down2))
    stat_copies = []
    for k in range(1, n):
        copy = pltpu.make_async_remote_copy(
            stats.at[me], stats.at[me], stat_send.at[k], stat_recv.at[me],
            device_id={"seq": lax.rem(me + k, n)}, device_id_type=MESH)
        copy.start()
        stat_copies.append(copy)

    launch(SENDS)

    def stat_wait(src):
        pltpu.make_async_remote_copy(
            stats.at[src], stats.at[src], stat_send.at[0], stat_recv.at[src],
            device_id={"seq": me}, device_id_type=MESH).wait_recv()

    def combine():
        for k in range(1, n):
            stat_wait(lax.rem(me + k, n))
        count = tokens * per_group
        every = [stats[k] for k in range(n)]
        mean = functools.reduce(jnp.add, [s[:1] for s in every]) * (1.0 / n)
        dev = functools.reduce(jnp.add, [s[1:2] + count * jnp.square(s[:1] - mean) for s in every])
        inv = lax.rsqrt(dev * (1.0 / (count * n)) + norm_eps)

        def stand(row):
            return jnp.transpose(jnp.broadcast_to(row, (LANES, LANES)))

        standing = split3(jnp.concatenate([stand(mean), stand(inv)], axis=1))
        columns = functools.reduce(jnp.add, [mm(expand[...], part3) for part3 in standing])
        mean_bc[...] = columns[:, :LANES]
        inv_bc[...] = columns[:, LANES:] * gain_col[...]

    def wide(block, width):
        return jnp.concatenate([block] * (width // LANES), axis=1)

    def project_norm(blocks):
        width = tokens * len(blocks)
        scaled = jnp.concatenate([
            ((block.astype(F32) - wide(mean_bc[...], tokens)) * wide(inv_bc[...], tokens)).astype(BF16)
            for block in blocks], axis=1)
        inner = mm(proj_in_w[...], scaled)
        centred = inner - jnp.mean(inner, axis=0, keepdims=True)
        spread = jnp.mean(jnp.square(centred), axis=0, keepdims=True)
        return inner, (centred * lax.rsqrt(spread + layer_eps) * wide(layer_col[...], width)).astype(BF16)

    in_first = lax.broadcasted_iota(jnp.int32, (pair_dim, tokens), 0) < head_dim

    def own_queries():
        inner, normed = project_norm([gathered[a, b]])
        inner_own[...] = inner
        scale = math.log2(math.e) / math.sqrt(head_dim)
        queries = mm(query_w[...], normed) * scale
        for p in range(pairs):
            rows = queries[p * pair_dim:(p + 1) * pair_dim]
            qbd[p] = jnp.concatenate(
                [jnp.where(in_first, rows, 0.0), jnp.where(in_first, 0.0, rows)], axis=1).astype(BF16)
        top[...] = jnp.full(top.shape, LOWEST, F32)
        total[...] = jnp.zeros(total.shape, F32)
        acc[...] = jnp.zeros(acc.shape, F32)

    group = 2 if rows_b % 2 == 0 else 1
    chunk = group * tokens
    kv_copies = []

    def beside(aa):
        for h in range(PIECES):
            for k in range(1, rows_b):
                arrive(aa, lax.rem(b + k, rows_b), h)

    def make_kv(aa):
        for i in range(rows_b // group):
            normed = project_norm([gathered[aa, i * group + j] for j in range(group)])[1]
            keys = mm(key_w[...], normed).astype(BF16)
            vbuf[aa, core, :, i * chunk:(i + 1) * chunk] = mm(value_w[...], normed).astype(BF16)
            for p in range(pairs):
                kbuf[aa, core, p, i * chunk:(i + 1) * chunk] = jnp.transpose(keys[p * pair_dim:(p + 1) * pair_dim])
        for slot, buf in enumerate((kbuf, vbuf)):
            copy = pltpu.make_async_remote_copy(
                buf.at[aa, core], buf.at[aa, core], kv_send.at[aa, slot], kv_recv.at[aa, slot],
                device_id={"seq": device(a, b, 1 - core)}, device_id_type=MESH)
            copy.start()
            kv_copies.append(copy)

    def partner_kv(aa):
        for slot, buf in enumerate((kbuf, vbuf)):
            pltpu.make_async_remote_copy(
                buf.at[aa, 1 - core], buf.at[aa, 1 - core], kv_send.at[aa, slot], kv_recv.at[aa, slot],
                device_id={"seq": device(a, b, 1 - core)}, device_id_type=MESH).wait_recv()

    def attend(parts):
        for i in range(rows_b // group):
            span = slice(i * chunk, (i + 1) * chunk)
            scores = [[mm(kbuf[aa, side, p, span], qbd[p]) for aa, side in parts] for p in range(pairs)]
            for p in range(pairs):
                before = top[p]
                peaks = [jnp.max(s, axis=0, keepdims=True) for s in scores[p]]
                now = functools.reduce(jnp.maximum, peaks, before)
                weights = [jnp.exp2(s - now) for s in scores[p]]
                fade = jnp.exp2(before - now)
                total[p] = total[p] * fade + functools.reduce(
                    jnp.add, [jnp.sum(w, axis=0, keepdims=True) for w in weights])
                top[p] = now
                mixes = [mm(vbuf[aa, side, p * pair_dim:(p + 1) * pair_dim, span], w.astype(BF16))
                         for (aa, side), w in zip(parts, weights)]
                acc[p] = acc[p] * fade + functools.reduce(jnp.add, mixes)

    table = row_order(rows_a)
    order = [sum(table[a0][k] * as_int(a == a0) for a0 in range(rows_a)) for k in range(rows_a)]
    def plan(words):
        for word in words:
            kind, arg = word[0], word[1:]
            if kind == "r":
                if int(arg) < rows_a:
                    relay(int(arg))
            elif kind == "s":
                combine()
            elif kind == "q":
                own_queries()
            elif int(arg[0]) >= rows_a:
                pass
            elif kind == "x":
                beside(order[int(arg)])
            elif kind == "k":
                make_kv(order[int(arg)])
            elif kind == "w":
                partner_kv(order[int(arg)])
            else:
                attend([(order[int(t[1])], core if t[0] == "o" else 1 - core)
                        for t in (word[j:j + 2] for j in range(0, len(word), 2)) if int(t[1]) < rows_a])

    plan(PLAN)

    mixed = []
    for p in range(pairs):
        ratio = acc[p] / total[p]
        mixed.append(jnp.where(in_first, ratio[:, :tokens], ratio[:, tokens:]))
    mixed = jnp.concatenate(mixed, axis=0).astype(BF16)
    after = (inner_own[...] + mm(attn_w[...], mixed)).astype(BF16)
    out[...] = (gathered[a, b].astype(F32) + mm(proj_w[...], after)).astype(BF16)

    pl.when(me < n - 1)(to_next.wait_send)
    pl.when(me > 0)(to_prev.wait_send)
    for copy in stat_copies + kv_copies:
        copy.wait_send()
    for cond, copy in pending:
        when(cond, copy.wait_send)


def local(
    n, features, hint, conv_weight, conv_bias, zero_weight, zero_bias, group_gain, proj_in,
    norm_gain, query_weight, key_weight, value_weight, attn_out, proj_out,
):
    tokens, channels = features.shape
    chips = n // CORES
    rows_a = math.gcd(chips, 4)
    rows_b = chips // rows_a
    pairs = HEADS // 2
    pair_dim = channels // pairs
    sends = PIECES * (8 * rows_b + 2 * (rows_a - 1) * rows_b)
    square = pltpu.VMEM((channels, channels), BF16)
    vector = pltpu.VMEM((channels,), F32)
    block = pltpu.VMEM((channels, tokens), BF16)
    column = pltpu.VMEM((channels, LANES), F32)
    hbm = pl.BlockSpec(memory_space=pltpu.HBM)
    result = pl.pallas_call(
        functools.partial(block_kernel, n, rows_a, rows_b),
        out_shape=jax.ShapeDtypeStruct((channels, tokens), BF16),
        in_specs=[hbm] * 14,
        out_specs=pl.BlockSpec(memory_space=pltpu.VMEM),
        scratch_shapes=[
            block, block, vector, vector, vector, vector,
            pltpu.VMEM(conv_weight.shape, BF16), square, square, square, square, square, square, square,
            pltpu.VMEM((2, channels, WIDTH), BF16),
            pltpu.VMEM((rows_a, rows_b, channels, tokens), BF16),
            pltpu.VMEM((rows_a, CORES, pairs, rows_b * tokens, pair_dim), BF16),
            pltpu.VMEM((rows_a, CORES, channels, rows_b * tokens), BF16),
            pltpu.VMEM((pairs, pair_dim, 2 * tokens), BF16),
            pltpu.VMEM((n, 2, LANES), F32),
            square,
            pltpu.VMEM((channels, LANES), BF16),
            column, column, column, column, column,
            pltpu.VMEM((channels, tokens), F32),
            pltpu.VMEM((pairs, 1, 2 * tokens), F32),
            pltpu.VMEM((pairs, 1, 2 * tokens), F32),
            pltpu.VMEM((pairs, pair_dim, 2 * tokens), F32),
            pltpu.SemaphoreType.DMA((14,)),
            pltpu.SemaphoreType.DMA((2,)),
            pltpu.SemaphoreType.DMA((2,)),
            pltpu.SemaphoreType.REGULAR((2,)),
            pltpu.SemaphoreType.DMA((n,)),
            pltpu.SemaphoreType.DMA((n,)),
            pltpu.SemaphoreType.DMA((sends,)),
            pltpu.SemaphoreType.DMA((rows_a, rows_b, PIECES)),
            pltpu.SemaphoreType.DMA((rows_a, 2)),
            pltpu.SemaphoreType.DMA((rows_a, 2)),
        ],
        compiler_params=pltpu.CompilerParams(
            collective_id=0, has_side_effects=True, vmem_limit_bytes=40 * 1024 * 1024),
    )(*(pltpu.with_memory_space_constraint(x, pltpu.HBM) for x in (
        features.T, hint.T, conv_bias, zero_bias, group_gain, norm_gain,
        conv_weight, zero_weight, proj_in, query_weight, key_weight, value_weight, attn_out, proj_out)))
    return result.T


def solution(mesh):
    split = P(("dp", "seq"), None)
    return jax.shard_map(
        functools.partial(local, mesh.shape["seq"]), mesh=mesh,
        in_specs=(split, split) + (P(),) * 12, out_specs=split, check_vma=False,
    )
```

```python
import functools
import math

import jax
import jax.numpy as jnp
from jax import lax
from jax.experimental import pallas as pl
from jax.experimental.pallas import tpu as pltpu
from jax.sharding import PartitionSpec as P

HEADS = 8
GROUPS = 32
WIDTH = 128
CORES = 2
LANES = 128
PIECES = 2
PLAN = (
    "r1", "s", "q", "x0", "k0", "r2", "r3", "o0", "w0", "x1", "k1", "p0o1", "x2", "k2",
    "w1", "p1o2", "x3", "k3", "w2", "p2o3", "w3", "p3",
)
EARLY = ()
SENDS = ("3","1","s")

norm_eps = 1e-06
layer_eps = 1e-05
MESH = pl.DeviceIdType.MESH
F32 = jnp.float32
BF16 = jnp.bfloat16
LOWEST = -3.0e38


def mm(x, y):
    return jnp.dot(x, y, preferred_element_type=F32)


def mm_t(x, y):
    return lax.dot_general(x, y, (((1,), (1,)), ((), ())), preferred_element_type=F32)


def split3(x):
    hi = x.astype(BF16)
    rest = x - hi.astype(F32)
    mid = rest.astype(BF16)
    lo = (rest - mid.astype(F32)).astype(BF16)
    return hi, mid, lo


def row_order(rows_a):
    return [sorted(range(rows_a), key=lambda aa: (abs(aa - a), abs(2 * aa - rows_a + 1))) for a in range(rows_a)]


def block_kernel(
    n, rows_a, rows_b,
    features_hbm, hint_hbm, conv_bias_hbm, zero_bias_hbm, group_gain_hbm, norm_gain_hbm,
    conv_hbm, zero_hbm, proj_in_hbm, query_hbm, key_hbm, value_hbm, attn_hbm, proj_hbm,
    out,
    features, hint, conv_bias, zero_bias, group_gain, norm_gain,
    conv_w, zero_w, proj_in_w, query_w, key_w, value_w, attn_w, proj_w,
    halo, gathered, kbuf, vbuf, qbd, stats, same, expand, zero_col, gain_col, layer_col, mean_bc, inv_bc,
    inner_own, top, total, acc,
    load_sem, halo_send, halo_recv, token, stat_send, stat_recv, send_sem, recv_sem, kv_send, kv_recv,
):
    channels, tokens = out.shape
    head_dim = channels // HEADS
    per_group = channels // GROUPS
    pairs = HEADS // 2
    pair_dim = 2 * head_dim
    me = lax.axis_index("seq")
    core = lax.rem(me, CORES)
    chip = lax.div(me, CORES)
    b = lax.rem(chip, rows_b)
    a = lax.div(chip, rows_b)

    def device(aa, bb, cc):
        return (aa * rows_b + bb) * CORES + cc

    loads = {}
    for slot, (name, src, dst) in enumerate((
        ("hint", hint_hbm, hint), ("conv", conv_hbm, conv_w), ("zero", zero_hbm, zero_w),
        ("features", features_hbm, features), ("conv_bias", conv_bias_hbm, conv_bias),
        ("zero_bias", zero_bias_hbm, zero_bias), ("group_gain", group_gain_hbm, group_gain),
        ("norm_gain", norm_gain_hbm, norm_gain), ("proj_in", proj_in_hbm, proj_in_w),
        ("query", query_hbm, query_w), ("key", key_hbm, key_w), ("value", value_hbm, value_w),
        ("attn", attn_hbm, attn_w), ("proj", proj_hbm, proj_w),
    )):
        loads[name] = pltpu.make_async_copy(src, dst, load_sem.at[slot])
        loads[name].start()

    pending = []

    def when(cond, fn):
        if cond is None:
            fn()
        else:
            pl.when(cond)(fn)

    def signal(sem, peer):
        pl.semaphore_signal(sem, inc=1, device_id={"seq": peer}, device_id_type=MESH)

    up, down = a < rows_a - 1, a > 0

    def as_int(cond):
        return cond.astype(jnp.int32)

    barrier = pltpu.get_barrier_semaphore()
    last_in_row = (b == rows_b - 1) & (core == 1) & up
    first_in_row = (b == 0) & (core == 0) & down
    mates = [(k, j) for k in range(rows_b) for j in range(CORES) if (k, j) != (0, 0)]
    for k, j in mates:
        signal(barrier, device(a, lax.rem(b + k, rows_b), lax.rem(core + j, CORES)))
    for cond, peer in ((up, device(a + 1, b, core)), (down, device(a - 1, b, core)),
                       (last_in_row, me + 1), (first_in_row, me - 1)):
        when(cond, functools.partial(signal, barrier, peer))
    pl.semaphore_wait(barrier, len(mates) + as_int(up) + as_int(down) + as_int(last_in_row) + as_int(first_in_row))

    loads["hint"].wait()
    to_next = pltpu.make_async_remote_copy(
        hint.at[:, pl.ds(tokens - WIDTH, WIDTH)], halo.at[0], halo_send.at[0], halo_recv.at[0], device_id={"seq": me + 1}, device_id_type=MESH)
    to_prev = pltpu.make_async_remote_copy(
        hint.at[:, pl.ds(0, WIDTH)], halo.at[1], halo_send.at[1], halo_recv.at[1], device_id={"seq": me - 1}, device_id_type=MESH)
    pl.when(me < n - 1)(to_next.start)
    pl.when(me > 0)(to_prev.start)

    when(up, functools.partial(signal, token.at[0], device(a + 1, b, core)))
    when(down, functools.partial(signal, token.at[0], device(a - 1, b, core)))

    @pl.when(me == 0)
    def _():
        halo[0] = jnp.zeros((channels, WIDTH), BF16)

    @pl.when(me == n - 1)
    def _():
        halo[1] = jnp.zeros((channels, WIDTH), BF16)

    row_group = lax.div(lax.broadcasted_iota(jnp.int32, (channels, channels), 0), jnp.int32(per_group))
    col_group = lax.div(lax.broadcasted_iota(jnp.int32, (channels, channels), 1), jnp.int32(per_group))
    same[...] = (row_group == col_group).astype(BF16)
    expand[...] = (
        lax.div(lax.broadcasted_iota(jnp.int32, (channels, LANES), 0), jnp.int32(per_group))
        == lax.broadcasted_iota(jnp.int32, (channels, LANES), 1)).astype(BF16)

    def as_columns(vector):
        return jnp.transpose(jnp.broadcast_to(vector[...].reshape(1, channels), (LANES, channels)))

    loads["conv"].wait()
    middle = jnp.transpose(hint[...])
    taps = [mm(middle, conv_w[1, d]) for d in range(3)]
    for name in ("zero", "features", "conv_bias", "zero_bias", "group_gain", "norm_gain"):
        loads[name].wait()
    zero_w[...] = jnp.transpose(zero_w[...])
    zero_col[...] = as_columns(zero_bias)
    gain_col[...] = as_columns(group_gain)
    layer_col[...] = as_columns(norm_gain)
    for name in ("proj_in", "query", "key", "value", "attn", "proj"):
        loads[name].wait()
    for weight in (proj_in_w, query_w, key_w, value_w, attn_w, proj_w):
        weight[...] = jnp.transpose(weight[...])

    pl.semaphore_wait(token.at[0], as_int(up) + as_int(down))
    up2, down2 = a + 2 < rows_a, a >= 2
    when(up2, functools.partial(signal, token.at[1], device(a + 2, b, core)))
    when(down2, functools.partial(signal, token.at[1], device(a - 2, b, core)))

    def line(k):
        rows = jnp.transpose(halo[k])
        if tokens > WIDTH:
            rows = jnp.where(
                k == 0, jnp.concatenate([rows, middle[:-WIDTH]], axis=0),
                jnp.concatenate([middle[WIDTH:], rows], axis=0))
        return rows

    pl.when(core == 0)(to_prev.wait_recv)
    pl.when(core == 1)(to_next.wait_recv)
    rows = line(1 - core)
    taps = [taps[d] + mm(rows, conv_w[2 - 2 * core, d]) for d in range(3)]
    pl.when((core == 0) & (me > 0))(to_next.wait_recv)
    pl.when((core == 1) & (me < n - 1))(to_prev.wait_recv)
    rows = line(core)
    taps = [taps[d] + mm(rows, conv_w[2 * core, d]) for d in range(3)]
    column = lax.rem(lax.broadcasted_iota(jnp.int32, (tokens, channels), 0), WIDTH)
    left = jnp.where(column == 0, 0.0, pltpu.roll(taps[0], 1, 0))
    right = jnp.where(column == WIDTH - 1, 0.0, pltpu.roll(taps[2], tokens - 1, 0))
    conv = left + taps[1] + right + conv_bias[...].reshape(1, channels)
    control = (conv / (1.0 + jnp.exp(-conv))).astype(BF16)
    branch = mm_t(zero_w[...], control) + zero_col[...]
    merged = (features[...].astype(F32) + branch).astype(BF16)
    gathered[a, b] = merged

    part = channels // PIECES

    def piece(aa, bb, h):
        return gathered.at[aa, bb, pl.ds(h * part, part)]

    def send(aa, bb, h, target, cond):
        slot = len(pending)
        copy = pltpu.make_async_remote_copy(
            piece(aa, bb, h), piece(aa, bb, h), send_sem.at[slot], recv_sem.at[aa, bb, h],
            device_id={"seq": target}, device_id_type=MESH)
        pending.append((cond, copy))
        when(cond, copy.start)

    def arrive(aa, bb, h):
        pltpu.make_async_remote_copy(
            piece(aa, bb, h), piece(aa, bb, h), send_sem.at[0], recv_sem.at[aa, bb, h],
            device_id={"seq": me}, device_id_type=MESH).wait_recv()

    def across(aa, h, cond):
        for k in range(1, rows_b):
            send(aa, b, h, device(a, lax.rem(b + k, rows_b), core), cond)

    def relay(step):
        for h in range(PIECES):
            for sign, inside, more in ((1, a + step < rows_a, down), (-1, a >= step, up)):
                aa = a + sign * step
                pl.when(inside)(functools.partial(arrive, aa, b, h))
                if step + 1 < rows_a and str(step + 1) not in EARLY + SENDS:
                    send(aa, b, h, device(a - sign, b, core), inside & more)
                if str(step) + "x" not in EARLY + SENDS:
                    across(aa, h, inside)

    def direct(step, columns):
        for h in range(PIECES):
            for sign, inside in ((-1, a >= step), (1, a + step < rows_a)):
                for k in columns:
                    send(a, b, h, device(a + sign * step, lax.rem(b + k, rows_b), core), inside)

    def launch(words):
        for word in words:
            if word == "s":
                for h in range(PIECES):
                    across(a, h, None)
            else:
                direct(int(word[0]), range(1, rows_b) if word[1:] else range(1))

    launch(EARLY)

    by_token = jnp.transpose(merged).astype(F32)
    shift = by_token[:1]
    apart = by_token - shift
    first = jnp.sum(apart, axis=0, keepdims=True)
    second = jnp.sum(apart * apart, axis=0, keepdims=True)
    channel_mean = shift + first * (1.0 / tokens)
    channel_dev = jnp.maximum(second - first * first * (1.0 / tokens), 0.0)

    def stack_rows(rows):
        fill = 16 - len(rows)
        return jnp.concatenate(rows + [jnp.zeros((fill,) + rows[0].shape[1:], BF16)], axis=0)

    spread = mm(stack_rows(list(split3(channel_mean))), same[...])
    group_mean = jnp.sum(spread[:3], axis=0, keepdims=True) * (1.0 / per_group)
    off = channel_mean - group_mean
    group_dev = channel_dev + tokens * off * off
    packed = mm(stack_rows(list(split3(channel_mean)) + list(split3(group_dev))), expand[...])
    stats[me] = jnp.concatenate([
        jnp.sum(packed[:3], axis=0, keepdims=True) * (1.0 / per_group),
        jnp.sum(packed[3:6], axis=0, keepdims=True)], axis=0)

    pl.semaphore_wait(token.at[1], as_int(up2) + as_int(down2))
    stat_copies = []
    for k in range(1, n):
        copy = pltpu.make_async_remote_copy(
            stats.at[me], stats.at[me], stat_send.at[k], stat_recv.at[me],
            device_id={"seq": lax.rem(me + k, n)}, device_id_type=MESH)
        copy.start()
        stat_copies.append(copy)

    launch(SENDS)

    def stat_wait(src):
        pltpu.make_async_remote_copy(
            stats.at[src], stats.at[src], stat_send.at[0], stat_recv.at[src],
            device_id={"seq": me}, device_id_type=MESH).wait_recv()

    def combine():
        for k in range(1, n):
            stat_wait(lax.rem(me + k, n))
        count = tokens * per_group
        every = [stats[k] for k in range(n)]
        mean = functools.reduce(jnp.add, [s[:1] for s in every]) * (1.0 / n)
        dev = functools.reduce(jnp.add, [s[1:2] + count * jnp.square(s[:1] - mean) for s in every])
        inv = lax.rsqrt(dev * (1.0 / (count * n)) + norm_eps)

        def stand(row):
            return jnp.transpose(jnp.broadcast_to(row, (LANES, LANES)))

        standing = split3(jnp.concatenate([stand(mean), stand(inv)], axis=1))
        columns = functools.reduce(jnp.add, [mm(expand[...], part3) for part3 in standing])
        mean_bc[...] = columns[:, :LANES]
        inv_bc[...] = columns[:, LANES:] * gain_col[...]

    def wide(block, width):
        return jnp.concatenate([block] * (width // LANES), axis=1)

    def project_norm(blocks):
        width = tokens * len(blocks)
        scaled = jnp.concatenate([
            ((block.astype(F32) - wide(mean_bc[...], tokens)) * wide(inv_bc[...], tokens)).astype(BF16)
            for block in blocks], axis=1)
        inner = mm(proj_in_w[...], scaled)
        centred = inner - jnp.mean(inner, axis=0, keepdims=True)
        spread = jnp.mean(jnp.square(centred), axis=0, keepdims=True)
        return inner, (centred * lax.rsqrt(spread + layer_eps) * wide(layer_col[...], width)).astype(BF16)

    in_first = lax.broadcasted_iota(jnp.int32, (pair_dim, tokens), 0) < head_dim

    def own_queries():
        inner, normed = project_norm([gathered[a, b]])
        inner_own[...] = inner
        scale = math.log2(math.e) / math.sqrt(head_dim)
        queries = mm(query_w[...], normed) * scale
        for p in range(pairs):
            rows = queries[p * pair_dim:(p + 1) * pair_dim]
            qbd[p] = jnp.concatenate(
                [jnp.where(in_first, rows, 0.0), jnp.where(in_first, 0.0, rows)], axis=1).astype(BF16)
        top[...] = jnp.full(top.shape, LOWEST, F32)
        total[...] = jnp.zeros(total.shape, F32)
        acc[...] = jnp.zeros(acc.shape, F32)

    group = 2 if rows_b % 2 == 0 else 1
    chunk = group * tokens
    kv_copies = []

    def beside(aa):
        for h in range(PIECES):
            for k in range(1, rows_b):
                arrive(aa, lax.rem(b + k, rows_b), h)

    def make_kv(aa):
        for i in range(rows_b // group):
            normed = project_norm([gathered[aa, i * group + j] for j in range(group)])[1]
            keys = mm(key_w[...], normed).astype(BF16)
            vbuf[aa, core, :, i * chunk:(i + 1) * chunk] = mm(value_w[...], normed).astype(BF16)
            for p in range(pairs):
                kbuf[aa, core, p, i * chunk:(i + 1) * chunk] = jnp.transpose(keys[p * pair_dim:(p + 1) * pair_dim])
        for slot, buf in enumerate((kbuf, vbuf)):
            copy = pltpu.make_async_remote_copy(
                buf.at[aa, core], buf.at[aa, core], kv_send.at[aa, slot], kv_recv.at[aa, slot],
                device_id={"seq": device(a, b, 1 - core)}, device_id_type=MESH)
            copy.start()
            kv_copies.append(copy)

    def partner_kv(aa):
        for slot, buf in enumerate((kbuf, vbuf)):
            pltpu.make_async_remote_copy(
                buf.at[aa, 1 - core], buf.at[aa, 1 - core], kv_send.at[aa, slot], kv_recv.at[aa, slot],
                device_id={"seq": device(a, b, 1 - core)}, device_id_type=MESH).wait_recv()

    def attend(parts):
        for i in range(rows_b // group):
            span = slice(i * chunk, (i + 1) * chunk)
            scores = [[mm(kbuf[aa, side, p, span], qbd[p]) for aa, side in parts] for p in range(pairs)]
            for p in range(pairs):
                before = top[p]
                peaks = [jnp.max(s, axis=0, keepdims=True) for s in scores[p]]
                now = functools.reduce(jnp.maximum, peaks, before)
                weights = [jnp.exp2(s - now) for s in scores[p]]
                fade = jnp.exp2(before - now)
                total[p] = total[p] * fade + functools.reduce(
                    jnp.add, [jnp.sum(w, axis=0, keepdims=True) for w in weights])
                top[p] = now
                mixes = [mm(vbuf[aa, side, p * pair_dim:(p + 1) * pair_dim, span], w.astype(BF16))
                         for (aa, side), w in zip(parts, weights)]
                acc[p] = acc[p] * fade + functools.reduce(jnp.add, mixes)

    table = row_order(rows_a)
    order = [sum(table[a0][k] * as_int(a == a0) for a0 in range(rows_a)) for k in range(rows_a)]
    def plan(words):
        for word in words:
            kind, arg = word[0], word[1:]
            if kind == "r":
                if int(arg) < rows_a:
                    relay(int(arg))
            elif kind == "s":
                combine()
            elif kind == "q":
                own_queries()
            elif int(arg[0]) >= rows_a:
                pass
            elif kind == "x":
                beside(order[int(arg)])
            elif kind == "k":
                make_kv(order[int(arg)])
            elif kind == "w":
                partner_kv(order[int(arg)])
            else:
                attend([(order[int(t[1])], core if t[0] == "o" else 1 - core)
                        for t in (word[j:j + 2] for j in range(0, len(word), 2)) if int(t[1]) < rows_a])

    plan(PLAN)

    mixed = []
    for p in range(pairs):
        ratio = acc[p] / total[p]
        mixed.append(jnp.where(in_first, ratio[:, :tokens], ratio[:, tokens:]))
    mixed = jnp.concatenate(mixed, axis=0).astype(BF16)
    after = (inner_own[...] + mm(attn_w[...], mixed)).astype(BF16)
    out[...] = (gathered[a, b].astype(F32) + mm(proj_w[...], after)).astype(BF16)

    pl.when(me < n - 1)(to_next.wait_send)
    pl.when(me > 0)(to_prev.wait_send)
    for copy in stat_copies + kv_copies:
        copy.wait_send()
    for cond, copy in pending:
        when(cond, copy.wait_send)


def local(
    n, features, hint, conv_weight, conv_bias, zero_weight, zero_bias, group_gain, proj_in,
    norm_gain, query_weight, key_weight, value_weight, attn_out, proj_out,
):
    tokens, channels = features.shape
    chips = n // CORES
    rows_a = math.gcd(chips, 4)
    rows_b = chips // rows_a
    pairs = HEADS // 2
    pair_dim = channels // pairs
    sends = PIECES * (8 * rows_b + 2 * (rows_a - 1) * rows_b)
    square = pltpu.VMEM((channels, channels), BF16)
    vector = pltpu.VMEM((channels,), F32)
    block = pltpu.VMEM((channels, tokens), BF16)
    column = pltpu.VMEM((channels, LANES), F32)
    hbm = pl.BlockSpec(memory_space=pltpu.HBM)
    result = pl.pallas_call(
        functools.partial(block_kernel, n, rows_a, rows_b),
        out_shape=jax.ShapeDtypeStruct((channels, tokens), BF16),
        in_specs=[hbm] * 14,
        out_specs=pl.BlockSpec(memory_space=pltpu.VMEM),
        scratch_shapes=[
            block, block, vector, vector, vector, vector,
            pltpu.VMEM(conv_weight.shape, BF16), square, square, square, square, square, square, square,
            pltpu.VMEM((2, channels, WIDTH), BF16),
            pltpu.VMEM((rows_a, rows_b, channels, tokens), BF16),
            pltpu.VMEM((rows_a, CORES, pairs, rows_b * tokens, pair_dim), BF16),
            pltpu.VMEM((rows_a, CORES, channels, rows_b * tokens), BF16),
            pltpu.VMEM((pairs, pair_dim, 2 * tokens), BF16),
            pltpu.VMEM((n, 2, LANES), F32),
            square,
            pltpu.VMEM((channels, LANES), BF16),
            column, column, column, column, column,
            pltpu.VMEM((channels, tokens), F32),
            pltpu.VMEM((pairs, 1, 2 * tokens), F32),
            pltpu.VMEM((pairs, 1, 2 * tokens), F32),
            pltpu.VMEM((pairs, pair_dim, 2 * tokens), F32),
            pltpu.SemaphoreType.DMA((14,)),
            pltpu.SemaphoreType.DMA((2,)),
            pltpu.SemaphoreType.DMA((2,)),
            pltpu.SemaphoreType.REGULAR((2,)),
            pltpu.SemaphoreType.DMA((n,)),
            pltpu.SemaphoreType.DMA((n,)),
            pltpu.SemaphoreType.DMA((sends,)),
            pltpu.SemaphoreType.DMA((rows_a, rows_b, PIECES)),
            pltpu.SemaphoreType.DMA((rows_a, 2)),
            pltpu.SemaphoreType.DMA((rows_a, 2)),
        ],
        compiler_params=pltpu.CompilerParams(
            collective_id=0, has_side_effects=True, vmem_limit_bytes=40 * 1024 * 1024),
    )(*(pltpu.with_memory_space_constraint(x, pltpu.HBM) for x in (
        features.T, hint.T, conv_bias, zero_bias, group_gain, norm_gain,
        conv_weight, zero_weight, proj_in, query_weight, key_weight, value_weight, attn_out, proj_out)))
    return result.T


def solution(mesh):
    split = P(("dp", "seq"), None)
    return jax.shard_map(
        functools.partial(local, mesh.shape["seq"]), mesh=mesh,
        in_specs=(split, split) + (P(),) * 12, out_specs=split, check_vma=False,
    )
```
